256 devices in a mesh: dish: 8 (over y_hi, x), chan: 32 (over y_lo, z, core).
Axes of the slice: x: 4, y: 4 (y_hi: 2, y_lo: 2; y = y_hi * 2 + y_lo), z: 8, core: 2. Of those that a mesh axis runs over, the one named last changes fastest.
Arguments:
- voltages: bfloat16 [2, 64, 4096, 512], P(None, 'dish', 'chan'), may hold values from -150 to 150
- beam_weights: bfloat16 [2, 4096, 64, 1024], P(None, ('chan', 'dish')), may hold values from -0.5 to 0.5
- flags: int32 [4096], P('chan'), may hold values 0 or 1
- sk_bins: int32 [4096], P('chan'), may hold values from 1 to 8
- bin_of_sample: int32 [512], replicated, may hold values from 0 to 63, never falling along the last dimension, each value on 1 to 16 neighbouring positions
Outputs:
- beam_power: bfloat16 [4096, 65536], P(None, ('dish', 'chan'))
The draws below stay inside these ranges and needn't reach their ends.
Inputs may be any that keep to these rules, and one draw needn't show every extreme that they name: `bin_of_sample`: never falls; each of the 64 bins holds 1 to 16 samples.
All inputs are finite; a program needn't handle non-finite values. No bound on the sum of `flags` on one device may be relied on, other than what follows from the above.
Results may differ from the reference program's by a relative error of at most 0.006.
Values may be sent and summed in bfloat16 or wider, within the bound.
No kernel may reach another device: no remote copies, remote signals or barrier semaphores. Data moves between devices by JAX's collectives and lax.ppermute only.
A program may use at most 64 MiB of HBM per device.

```python
import math
import jax
import jax.numpy as jnp
import numpy as np
from jax import lax

DISH = 64
CH = 4096
BEAMS = 1024
T_SIZE = 512
TBINS = 64


def draw_voltages(key, part):
    keys = jax.random.split(key, 4)
    base = jnp.clip(jax.random.normal(keys[0], (2, DISH, CH, T_SIZE), jnp.float32), -6.0, 6.0)
    ramped = 1.0 + 0.8 * jnp.arange(DISH, dtype=jnp.float32) / (DISH - 1)
    jitter = jnp.exp(jax.random.uniform(keys[1], (DISH,), jnp.float32, -0.15, 0.15))
    amplitude = ramped * jitter
    depth = jax.random.uniform(keys[2], (CH,), jnp.float32, 0.0, 0.35)
    swing = jnp.clip(jax.random.normal(keys[3], (CH, T_SIZE), jnp.float32), -4.0, 4.0)
    envelope = jnp.exp(depth[:, None] * swing)
    return (base * amplitude[None, :, None, None] * envelope[None, None]).astype(jnp.bfloat16)


def set_ends(values, own_key, smallest, top_value):
    index_at = [jax.random.randint(jax.random.fold_in(own_key, axis), (), 0, length) for axis, length in enumerate(values.shape)]
    widest = values.shape.index(max(values.shape))
    next_to = index_at[:widest] + [(index_at[widest] + 1) % values.shape[widest]] + index_at[widest + 1:]
    return values.at[tuple(index_at)].set(smallest).at[tuple(next_to)].set(top_value)


def shard_levels(own_key, extent, shards, smallest, top_value):
    gain = 1.0
    for axis_at, parts in shards:
        steps = jax.random.uniform(jax.random.fold_in(jax.random.fold_in(own_key, 6), axis_at), (parts,), jnp.float32, smallest / len(shards), top_value / len(shards))
        gain = gain * jnp.repeat(jnp.exp(steps), extent[axis_at] // parts).reshape((-1,) + (1,) * (len(extent) - 1 - axis_at))
    return gain


def length_profile(amount, total, most, slope):
    loads = [(1 << 20) // math.isqrt(standing ** slope) + 1 for standing in range(2, amount + 1)]
    surplus, given = total - most - (amount - 1), [1] * (amount - 1)
    while surplus > 0:
        movable = [i for i in range(amount - 1) if given[i] < most]
        mass, budget = sum([loads[i] for i in movable]), surplus
        for i in movable:
            extra = min(most - given[i], max(1, budget * loads[i] // mass), surplus)
            given[i] = given[i] + extra
            surplus = surplus - extra
    return np.array([most] + given)


def ragged(rng, count, total, reach, skew):
    if count == 2:
        one = jax.random.randint(rng, (), max(1, total - reach), min(reach, total - 1) + 1)
        return jnp.stack([one, total - one])
    lengths = jnp.asarray(length_profile(count, total, reach, skew), jnp.int32)
    pairs = (count - 1) // 2
    source_of, receiver = lengths[1:1 + 2 * pairs:2], lengths[2:2 + 2 * pairs:2]
    margin = jnp.minimum(source_of - 1, reach - receiver)
    moved = jax.random.randint(jax.random.fold_in(rng, 1), (pairs,), 0, 1 << 20) % (margin + 1)
    lengths = lengths.at[1:1 + 2 * pairs:2].set(source_of - moved).at[2:2 + 2 * pairs:2].set(receiver + moved)
    return lengths[jax.random.permutation(jax.random.fold_in(rng, 2), count)]


def gaussian(rng, shape, width, limit, pieces=(), held_as=jnp.bfloat16):
    result = width * jax.random.normal(rng, shape, jnp.float32)
    if pieces:
        result = result * shard_levels(rng, shape, pieces, -0.22, 0.18)
    return jnp.clip(result, -limit, limit).astype(held_as)


def setup_inputs(seed: int = 0) -> dict:
    seeds = jax.random.split(jax.random.key(seed), 6)
    return {
        "voltages": draw_voltages(jax.random.fold_in(seeds[5], 71), 0),
        "beam_weights": gaussian(seeds[1], (2, CH, DISH, BEAMS), (2 * DISH) ** -0.5, 0.5, ((1, 256),)),
        "flags": set_ends((jax.random.randint(seeds[2], (CH,), 0, 8) < 7).astype(jnp.int32), jax.random.fold_in(seeds[2], 1), 0, 1),
        "sk_bins": set_ends(jax.random.randint(seeds[3], (CH,), 1, 9), jax.random.fold_in(seeds[3], 1), 1, 8).astype(jnp.int32),
        "bin_of_sample": jnp.searchsorted(jnp.cumsum(ragged(seeds[4], TBINS, T_SIZE, 16, 1)), jnp.arange(T_SIZE), side="right").astype(jnp.int32),
    }


def kurtosis_scale(first_sum, second_sum, samples, flags, sk_bins):
    widths = 0.05 * sk_bins.astype(jnp.float32)
    mean_one = first_sum / samples
    mean_two = second_sum / samples
    ratio = mean_two / (mean_one * mean_one + 1e-6)
    kurtosis = (samples + 1.0) / (samples - 1.0) * (ratio - 1.0)
    excess = kurtosis - 1.0
    return flags.astype(jnp.float32) * widths / (widths + excess * excess)


def channel_average(volts, weights, onehot, counts):
    stacked_v = jnp.concatenate([volts[0], volts[1]], axis=0)
    real_rows = jnp.concatenate([weights[0], -weights[1]], axis=0)
    imag_rows = jnp.concatenate([weights[1], weights[0]], axis=0)
    stacked_w = jnp.concatenate([real_rows, imag_rows], axis=1)
    beam_volts = jnp.dot(stacked_w.T, stacked_v, preferred_element_type=jnp.float32)
    half = weights.shape[2]
    real_part = beam_volts[:half]
    imag_part = beam_volts[half:]
    powers = real_part * real_part + imag_part * imag_part
    upper = powers.astype(jnp.bfloat16)
    lower = (powers - upper.astype(jnp.float32)).astype(jnp.bfloat16)
    summed = jnp.dot(upper, onehot, preferred_element_type=jnp.float32) + jnp.dot(lower, onehot, preferred_element_type=jnp.float32)
    return summed / counts[None, :]


def reference(voltages, beam_weights, flags, sk_bins, bin_of_sample):
    floats = voltages.astype(jnp.float32)
    powers = floats[0] * floats[0] + floats[1] * floats[1]
    first_sum = jnp.sum(powers, axis=(0, 2))
    second_sum = jnp.sum(powers * powers, axis=(0, 2))
    samples = float(DISH * T_SIZE)
    scaling = kurtosis_scale(first_sum, second_sum, samples, flags, sk_bins)
    scaled = (floats * scaling[None, None, :, None]).astype(jnp.bfloat16)
    matches = bin_of_sample[:, None] == jnp.arange(TBINS, dtype=jnp.int32)[None, :]
    onehot = matches.astype(jnp.bfloat16)
    counts = jnp.sum(matches.astype(jnp.float32), axis=0)
    by_channel = jnp.moveaxis(scaled, 2, 0)
    weights_by = jnp.moveaxis(beam_weights, 1, 0)

    def one_channel(items):
        return channel_average(items[0], items[1], onehot, counts)

    averaged = lax.map(one_channel, (by_channel, weights_by))
    return averaged.reshape(CH, BEAMS * TBINS).astype(jnp.bfloat16)
```

```python
import functools

import jax
import jax.numpy as jnp
from jax import lax
from jax.experimental import pallas as pl
from jax.experimental.pallas import tpu as pltpu
from jax.sharding import PartitionSpec as P

TBINS = 64
CHUNKS = 1


def weight_rows_kernel(owners, weights_ref, rows_ref):
    per_owner = rows_ref.shape[1]
    span = rows_ref.shape[3]
    block = per_owner * span
    stacked = jnp.concatenate([weights_ref[0, 0], weights_ref[1, 0]], axis=0)
    new = lax.broadcasted_iota(jnp.int32, (block, block), 0)
    old = lax.broadcasted_iota(jnp.int32, (block, block), 1)
    wanted = (new % span) * per_owner + new // span
    pick = (wanted == old).astype(jnp.bfloat16)
    for at in range(owners):
        piece = stacked[:, at * block : (at + 1) * block]
        turned = lax.dot_general(
            pick, piece, (((1,), (1,)), ((), ())), preferred_element_type=jnp.float32
        ).astype(jnp.bfloat16)
        for j in range(per_owner):
            rows_ref[0, j, at] = turned[j * span : (j + 1) * span]


def weight_rows(weights, per_owner, dish_count, chan_count):
    _, chans, dishes, beams = weights.shape
    shape = (chans, per_owner, dish_count, chan_count, 2 * dishes)
    return pl.pallas_call(
        functools.partial(weight_rows_kernel, dish_count),
        grid=(chans,),
        in_specs=[pl.BlockSpec((2, 1, dishes, beams), lambda c: (0, c, 0, 0))],
        out_specs=pl.BlockSpec((1, *shape[1:]), lambda c: (c, 0, 0, 0, 0)),
        out_shape=jax.ShapeDtypeStruct(shape, jnp.bfloat16),
        cost_estimate=pl.CostEstimate(
            flops=2 * chans * beams * 128 * 2 * dishes,
            bytes_accessed=8 * chans * beams * dishes,
            transcendentals=0,
        ),
        name="weight_rows",
    )(weights)


def beam_kernel(samples, volts_ref, rows_ref, onehot_ref, inverse_ref, flag_ref, width_ref, out_ref):
    groups, _, _, inside, times = volts_ref.shape
    dishes = groups * inside
    real = volts_ref[:, 0, 0].reshape(dishes, times)
    imag = volts_ref[:, 0, 1].reshape(dishes, times)
    real_f, imag_f = real.astype(jnp.float32), imag.astype(jnp.float32)
    power = real_f * real_f + imag_f * imag_f
    first = jnp.sum(jnp.sum(power, axis=1, keepdims=True), axis=0, keepdims=True)
    second = jnp.sum(jnp.sum(power * power, axis=1, keepdims=True), axis=0, keepdims=True)
    mean_one = first / samples
    mean_two = second / samples
    ratio = mean_two / (mean_one * mean_one + 1e-06)
    kurtosis = (samples + 1.0) / (samples - 1.0) * (ratio - 1.0)
    excess = kurtosis - 1.0
    widths = width_ref[0]
    scaling = flag_ref[0] * widths / (widths + excess * excess)
    gain = (scaling * scaling) * inverse_ref[...]
    stacked = jnp.concatenate(
        [jnp.concatenate([real, imag], axis=1), jnp.concatenate([-imag, real], axis=1)], axis=0
    )
    summed = None
    for j in range(rows_ref.shape[1]):
        beams = jnp.dot(rows_ref[0, j], stacked, preferred_element_type=jnp.float32)
        re, im = beams[:, :times], beams[:, times:]
        detected = (re * re + im * im).astype(jnp.bfloat16)
        part = jnp.dot(detected, onehot_ref[j], preferred_element_type=jnp.float32)
        summed = part if summed is None else summed + part
    out_ref[0] = (summed * gain).astype(jnp.bfloat16)


def beam_power(samples, volts, rows, onehot, inverse, flag, width, first_chan):
    groups, chans, _, inside, times = volts.shape
    _, per_owner, owners, depth = rows.shape
    lanes = onehot.shape[2]
    whole = lambda *dims: pl.BlockSpec(dims, lambda c: (0,) * len(dims))
    return pl.pallas_call(
        functools.partial(beam_kernel, samples),
        grid=(chans,),
        in_specs=[
            pl.BlockSpec((groups, 1, 2, inside, times), lambda c: (0, c, 0, 0, 0)),
            pl.BlockSpec((1, per_owner, owners, depth), lambda c: (c + first_chan, 0, 0, 0)),
            whole(*onehot.shape),
            whole(*inverse.shape),
            pl.BlockSpec((1, 1, 1), lambda c: (c + first_chan, 0, 0)),
            pl.BlockSpec((1, 1, 1), lambda c: (c + first_chan, 0, 0)),
        ],
        out_specs=pl.BlockSpec((1, owners, lanes), lambda c: (c, 0, 0)),
        out_shape=jax.ShapeDtypeStruct((chans, owners, lanes), jnp.bfloat16),
        cost_estimate=pl.CostEstimate(
            flops=2 * chans * owners * per_owner * times * (2 * depth + lanes),
            bytes_accessed=2 * chans * (owners * per_owner * depth + depth * times + owners * lanes),
            transcendentals=0,
        ),
        name="beam_power",
    )(volts, rows, onehot, inverse, flag, width)


def body(voltages, beam_weights, flags, sk_bins, bin_of_sample):
    dish_count = lax.axis_size("dish")
    chan_count = lax.axis_size("chan")
    _, inside, chan_block, times = voltages.shape
    chans = chan_block // dish_count
    samples = float(inside * dish_count * times)
    owners = dish_count * chan_count
    per_owner = beam_weights.shape[3] // owners
    part = chans // CHUNKS

    by_peer = voltages.reshape(2, inside, dish_count, CHUNKS, part, times).transpose(3, 2, 4, 0, 1, 5)
    arrived = [
        lax.all_to_all(by_peer[k], "dish", split_axis=0, concat_axis=0, tiled=True)
        for k in range(CHUNKS)
    ]

    rows = weight_rows(beam_weights, per_owner, dish_count, chan_count)
    rows = rows.reshape(chans, per_owner, owners, -1)
    offset = lax.axis_index("dish") * chans
    flag = lax.dynamic_slice_in_dim(flags, offset, chans).astype(jnp.float32)
    width = 0.05 * lax.dynamic_slice_in_dim(sk_bins, offset, chans).astype(jnp.float32)
    matches = bin_of_sample[:, None] == jnp.arange(TBINS, dtype=jnp.int32)[None, :]
    inverse = jnp.tile(1.0 / jnp.sum(matches.astype(jnp.float32), axis=0), per_owner)[None, :]
    lane = jnp.arange(per_owner * TBINS, dtype=jnp.int32)
    place = jnp.arange(per_owner, dtype=jnp.int32)[:, None, None] * TBINS + bin_of_sample[None, :, None]
    onehot = (place == lane[None, None, :]).astype(jnp.bfloat16)

    moved = []
    for k in range(CHUNKS):
        power = beam_power(
            samples, arrived[k], rows, onehot, inverse, flag[:, None, None], width[:, None, None], k * part
        )
        blocks = power.reshape(part, dish_count, chan_count, -1).transpose(2, 1, 0, 3)
        blocks = blocks.reshape(owners, part, -1)
        moved.append(lax.all_to_all(blocks, ("chan", "dish"), split_axis=0, concat_axis=0, tiled=True))
    whole = jnp.concatenate(moved, axis=1)
    return whole.reshape(owners * chans, -1)


def solution(mesh):
    in_specs = (
        P(None, "dish", "chan", None),
        P(None, ("chan", "dish"), None, None),
        P("chan"),
        P("chan"),
        P(),
    )
    out_specs = P(None, ("dish", "chan"))
    return jax.shard_map(body, mesh=mesh, in_specs=in_specs, out_specs=out_specs, check_vma=False)
```

```python
import functools

import jax
import jax.numpy as jnp
from jax import lax
from jax.experimental import pallas as pl
from jax.experimental.pallas import tpu as pltpu
from jax.sharding import PartitionSpec as P

TBINS = 64
STEP = 4
ROW = 4
VMEM_LIMIT = 46 * 1024 * 1024


def member(place, count):
    return place % (count // ROW) * ROW + place // (count // ROW)


def weight_rows_kernel(owners, weights_ref, rows_ref):
    per_owner = rows_ref.shape[1]
    span = rows_ref.shape[3]
    block = per_owner * span
    inside = weights_ref.shape[2] // owners
    stacked = []
    for part in range(2):
        for place in range(owners):
            start = member(place, owners) * inside
            stacked.append(weights_ref[part, 0, start : start + inside, :])
    stacked = jnp.concatenate(stacked, axis=0)
    new = lax.broadcasted_iota(jnp.int32, (block, block), 0)
    old = lax.broadcasted_iota(jnp.int32, (block, block), 1)
    wanted = (new % span) * per_owner + new // span
    pick = (wanted == old).astype(jnp.bfloat16)
    for at in range(owners):
        piece = stacked[:, at * block : (at + 1) * block]
        turned = lax.dot_general(
            pick, piece, (((1,), (1,)), ((), ())), preferred_element_type=jnp.float32
        ).astype(jnp.bfloat16)
        for j in range(per_owner):
            rows_ref[0, j, at] = turned[j * span : (j + 1) * span]


def weight_rows(weights, per_owner, dish_count, chan_count):
    _, chans, dishes, beams = weights.shape
    shape = (chans, per_owner, dish_count, chan_count, 2 * dishes)
    return pl.pallas_call(
        functools.partial(weight_rows_kernel, dish_count),
        grid=(chans,),
        in_specs=[pl.BlockSpec((2, 1, dishes, beams), lambda c: (0, c, 0, 0))],
        out_specs=pl.BlockSpec((1, *shape[1:]), lambda c: (c, 0, 0, 0, 0)),
        out_shape=jax.ShapeDtypeStruct(shape, jnp.bfloat16),
        compiler_params=pltpu.CompilerParams(vmem_limit_bytes=VMEM_LIMIT),
        cost_estimate=pl.CostEstimate(
            flops=2 * chans * beams * 128 * 2 * dishes,
            bytes_accessed=8 * chans * beams * dishes,
            transcendentals=0,
        ),
        name="weight_rows",
    )(weights)


def channel_power(samples, at, volts_ref, rows_ref, onehot_ref, inverse_ref, flag_ref, width_ref):
    groups, _, _, inside, times = volts_ref.shape
    dishes = groups * inside
    real = volts_ref[:, at, 0].reshape(dishes, times)
    imag = volts_ref[:, at, 1].reshape(dishes, times)
    real_f, imag_f = real.astype(jnp.float32), imag.astype(jnp.float32)
    power = real_f * real_f + imag_f * imag_f
    first = jnp.sum(jnp.sum(power, axis=1, keepdims=True), axis=0, keepdims=True)
    second = jnp.sum(jnp.sum(power * power, axis=1, keepdims=True), axis=0, keepdims=True)
    mean_one = first / samples
    mean_two = second / samples
    ratio = mean_two / (mean_one * mean_one + 1e-06)
    kurtosis = (samples + 1.0) / (samples - 1.0) * (ratio - 1.0)
    excess = kurtosis - 1.0
    widths = width_ref[at]
    scaling = flag_ref[at] * widths / (widths + excess * excess)
    gain = (scaling * scaling) * inverse_ref[...]
    stacked = jnp.concatenate(
        [jnp.concatenate([real, imag], axis=1), jnp.concatenate([-imag, real], axis=1)], axis=0
    )
    detected = []
    for j in range(rows_ref.shape[1]):
        beams = jnp.dot(rows_ref[at, j], stacked, preferred_element_type=jnp.float32)
        re, im = beams[:, :times], beams[:, times:]
        detected.append((re * re + im * im).astype(jnp.bfloat16))
    summed = jnp.dot(
        jnp.concatenate(detected, axis=1), onehot_ref[...], preferred_element_type=jnp.float32
    )
    return summed * gain


def beam_kernel(samples, *refs):
    *operands, out_ref = refs
    for at in range(STEP):
        out_ref[at] = channel_power(samples, at, *operands).astype(jnp.bfloat16)


def beam_power(samples, volts, rows, onehot, inverse, flag, width):
    groups, chans, _, inside, times = volts.shape
    _, per_owner, owners, depth = rows.shape
    lanes = onehot.shape[1]
    whole = lambda *dims: pl.BlockSpec(dims, lambda c: (0,) * len(dims))
    return pl.pallas_call(
        functools.partial(beam_kernel, samples),
        grid=(chans // STEP,),
        in_specs=[
            pl.BlockSpec((groups, STEP, 2, inside, times), lambda c: (0, c, 0, 0, 0)),
            pl.BlockSpec((STEP, per_owner, owners, depth), lambda c: (c, 0, 0, 0)),
            whole(*onehot.shape),
            whole(*inverse.shape),
            pl.BlockSpec((STEP, 1, 1), lambda c: (c, 0, 0)),
            pl.BlockSpec((STEP, 1, 1), lambda c: (c, 0, 0)),
        ],
        out_specs=pl.BlockSpec((STEP, owners, lanes), lambda c: (c, 0, 0)),
        out_shape=jax.ShapeDtypeStruct((chans, owners, lanes), jnp.bfloat16),
        compiler_params=pltpu.CompilerParams(vmem_limit_bytes=VMEM_LIMIT),
        cost_estimate=pl.CostEstimate(
            flops=2 * chans * owners * per_owner * times * (2 * depth + lanes),
            bytes_accessed=2 * chans * (owners * per_owner * depth + depth * times + owners * lanes),
            transcendentals=0,
        ),
        name="beam_power",
    )(volts, rows, onehot, inverse, flag, width)


def body(voltages, beam_weights, flags, sk_bins, bin_of_sample):
    dish_count = lax.axis_size("dish")
    chan_count = lax.axis_size("chan")
    _, inside, chan_block, times = voltages.shape
    chans = chan_block // dish_count
    samples = float(inside * dish_count * times)
    owners = dish_count * chan_count
    per_owner = beam_weights.shape[3] // owners

    by_peer = voltages.reshape(2, inside, dish_count // ROW, ROW, chans, times)
    arrived = lax.all_to_all(
        by_peer.transpose(3, 2, 4, 0, 1, 5).reshape(dish_count, chans, 2, inside, times),
        "dish",
        split_axis=0,
        concat_axis=0,
        tiled=True,
        axis_index_groups=[[member(i, dish_count) for i in range(dish_count)]],
    )

    rows = weight_rows(beam_weights, per_owner, dish_count, chan_count)
    rows = rows.reshape(chans, per_owner, owners, -1)
    offset = lax.axis_index("dish") * chans
    flag = lax.dynamic_slice_in_dim(flags, offset, chans).astype(jnp.float32)
    width = 0.05 * lax.dynamic_slice_in_dim(sk_bins, offset, chans).astype(jnp.float32)
    matches = bin_of_sample[:, None] == jnp.arange(TBINS, dtype=jnp.int32)[None, :]
    inverse = jnp.tile(1.0 / jnp.sum(matches.astype(jnp.float32), axis=0), per_owner)[None, :]
    lane = jnp.arange(per_owner * TBINS, dtype=jnp.int32)
    place = jnp.arange(per_owner, dtype=jnp.int32)[:, None, None] * TBINS + bin_of_sample[None, :, None]
    onehot = (place == lane[None, None, :]).astype(jnp.bfloat16).reshape(per_owner * times, -1)

    power = beam_power(
        samples, arrived, rows, onehot, inverse, flag[:, None, None], width[:, None, None]
    )
    blocks = power.reshape(chans, dish_count, chan_count, -1).transpose(2, 1, 0, 3)
    moved = lax.all_to_all(
        blocks.reshape(owners, chans, -1), ("chan", "dish"), split_axis=0, concat_axis=0, tiled=True
    )
    return moved.reshape(owners * chans, -1)


def solution(mesh):
    in_specs = (
        P(None, "dish", "chan", None),
        P(None, ("chan", "dish"), None, None),
        P("chan"),
        P("chan"),
        P(),
    )
    out_specs = P(None, ("dish", "chan"))
    return jax.shard_map(body, mesh=mesh, in_specs=in_specs, out_specs=out_specs, check_vma=False)
```

```python
import functools

import jax
import jax.numpy as jnp
from jax import lax
from jax.experimental import pallas as pl
from jax.experimental.pallas import tpu as pltpu
from jax.sharding import PartitionSpec as P

TBINS = 64
STEP = 4
ROW = 4
DISHES = 8
LANES = 128
VMEM_LIMIT = 46 * 1024 * 1024


def relative(index, step, sign):
    rows = DISHES // ROW
    across = (index % ROW + sign * (step % ROW) + ROW) % ROW
    return (index // ROW + step // ROW) % rows * ROW + across


def distance(step):
    across = step % ROW
    return 4 * (step // ROW) + min(across, ROW - across)


def turn_kernel(order, me_ref, volts_ref, *refs):
    *outs, floats_ref = refs
    parts, inside, _, times = volts_ref.shape
    count = len(outs)
    chans = outs[0].shape[0]
    for k in range(count):
        start = pl.multiple_of(relative(me_ref[0], order[k], 1) * chans, chans)
        block = volts_ref[:, :, pl.ds(start, chans), :].astype(jnp.float32)
        block = block.reshape(parts * inside * chans, times)
        for tile in range(times // LANES):
            lanes = slice(tile * LANES, (tile + 1) * LANES)
            floats_ref[k % 2, tile] = block[:, lanes]
        for tile in range(times // LANES):
            lanes = slice(tile * LANES, (tile + 1) * LANES)
            for chan in range(chans):
                rows = floats_ref[k % 2, tile, pl.ds(chan, parts * inside, stride=chans), :]
                outs[k][chan, :, lanes] = rows.astype(jnp.bfloat16)


def turned_blocks(volts, me, order):
    parts, inside, chan_block, times = volts.shape
    count = len(order)
    chans = chan_block // count
    shape = jax.ShapeDtypeStruct((chans, parts * inside, times), jnp.bfloat16)
    return pl.pallas_call(
        functools.partial(turn_kernel, order),
        in_specs=[pl.BlockSpec(memory_space=pltpu.SMEM), pl.BlockSpec(memory_space=pltpu.VMEM)],
        out_specs=[pl.BlockSpec(memory_space=pltpu.VMEM)] * count,
        out_shape=[shape] * count,
        scratch_shapes=[
            pltpu.VMEM((2, times // LANES, parts * inside * chans, LANES), jnp.float32)
        ],
        compiler_params=pltpu.CompilerParams(vmem_limit_bytes=VMEM_LIMIT),
        name="turned_blocks",
    )(me, volts)


def weight_rows_kernel(order, me_ref, weights_ref, rows_ref):
    owners = len(order)
    per_owner = rows_ref.shape[1]
    span = rows_ref.shape[3]
    block = per_owner * span
    inside = weights_ref.shape[2] // owners
    stacked = []
    for part in range(2):
        for step in order:
            start = pl.multiple_of(relative(me_ref[0], step, -1) * inside, inside)
            stacked.append(weights_ref[part, 0, pl.ds(start, inside), :])
    stacked = jnp.concatenate(stacked, axis=0)
    new = lax.broadcasted_iota(jnp.int32, (block, block), 0)
    old = lax.broadcasted_iota(jnp.int32, (block, block), 1)
    wanted = (new % span) * per_owner + new // span
    pick = (wanted == old).astype(jnp.bfloat16)
    for at in range(owners):
        piece = stacked[:, at * block : (at + 1) * block]
        turned = lax.dot_general(
            pick, piece, (((1,), (1,)), ((), ())), preferred_element_type=jnp.float32
        ).astype(jnp.bfloat16)
        for j in range(per_owner):
            rows_ref[0, j, at] = turned[j * span : (j + 1) * span]


def weight_rows(weights, me, order, per_owner, dish_count, chan_count):
    _, chans, dishes, beams = weights.shape
    shape = (chans, per_owner, dish_count, chan_count, 2 * dishes)
    return pl.pallas_call(
        functools.partial(weight_rows_kernel, order),
        grid=(chans,),
        in_specs=[
            pl.BlockSpec(memory_space=pltpu.SMEM),
            pl.BlockSpec((2, 1, dishes, beams), lambda c: (0, c, 0, 0)),
        ],
        out_specs=pl.BlockSpec((1, *shape[1:]), lambda c: (c, 0, 0, 0, 0)),
        out_shape=jax.ShapeDtypeStruct(shape, jnp.bfloat16),
        compiler_params=pltpu.CompilerParams(vmem_limit_bytes=VMEM_LIMIT),
        cost_estimate=pl.CostEstimate(
            flops=2 * chans * beams * 128 * 2 * dishes,
            bytes_accessed=8 * chans * beams * dishes,
            transcendentals=0,
        ),
        name="weight_rows",
    )(me, weights)


def channel_power(samples, at, refs):
    *volts_refs, rows_ref, onehot_ref, inverse_ref, flag_ref, width_ref = refs
    _, both, times = volts_refs[0].shape
    half = both // 2
    real = jnp.concatenate([ref[at, :half] for ref in volts_refs], axis=0)
    imag = jnp.concatenate([ref[at, half:] for ref in volts_refs], axis=0)
    real_f, imag_f = real.astype(jnp.float32), imag.astype(jnp.float32)
    power = real_f * real_f + imag_f * imag_f
    first = jnp.sum(jnp.sum(power, axis=1, keepdims=True), axis=0, keepdims=True)
    second = jnp.sum(jnp.sum(power * power, axis=1, keepdims=True), axis=0, keepdims=True)
    mean_one = first / samples
    mean_two = second / samples
    ratio = mean_two / (mean_one * mean_one + 1e-06)
    kurtosis = (samples + 1.0) / (samples - 1.0) * (ratio - 1.0)
    excess = kurtosis - 1.0
    widths = width_ref[at]
    scaling = flag_ref[at] * widths / (widths + excess * excess)
    gain = (scaling * scaling) * inverse_ref[...]
    stacked = jnp.concatenate(
        [jnp.concatenate([real, imag], axis=1), jnp.concatenate([-imag, real], axis=1)], axis=0
    )
    detected = []
    for j in range(rows_ref.shape[1]):
        beams = jnp.dot(rows_ref[at, j], stacked, preferred_element_type=jnp.float32)
        re, im = beams[:, :times], beams[:, times:]
        detected.append((re * re + im * im).astype(jnp.bfloat16))
    summed = jnp.dot(
        jnp.concatenate(detected, axis=1), onehot_ref[...], preferred_element_type=jnp.float32
    )
    return summed * gain


def beam_kernel(samples, *refs):
    *operands, out_ref = refs
    for at in range(STEP):
        out_ref[at] = channel_power(samples, at, operands).astype(jnp.bfloat16)


def beam_power(samples, volts, rows, onehot, inverse, flag, width):
    chans, both, times = volts[0].shape
    _, per_owner, owners, depth = rows.shape
    lanes = onehot.shape[1]
    whole = lambda *dims: pl.BlockSpec(dims, lambda c: (0,) * len(dims))
    return pl.pallas_call(
        functools.partial(beam_kernel, samples),
        grid=(chans // STEP,),
        in_specs=[
            *[pl.BlockSpec((STEP, both, times), lambda c: (c, 0, 0))] * len(volts),
            pl.BlockSpec((STEP, per_owner, owners, depth), lambda c: (c, 0, 0, 0)),
            whole(*onehot.shape),
            whole(*inverse.shape),
            pl.BlockSpec((STEP, 1, 1), lambda c: (c, 0, 0)),
            pl.BlockSpec((STEP, 1, 1), lambda c: (c, 0, 0)),
        ],
        out_specs=pl.BlockSpec((STEP, owners, lanes), lambda c: (c, 0, 0)),
        out_shape=jax.ShapeDtypeStruct((chans, owners, lanes), jnp.bfloat16),
        compiler_params=pltpu.CompilerParams(vmem_limit_bytes=VMEM_LIMIT),
        cost_estimate=pl.CostEstimate(
            flops=2 * chans * owners * per_owner * times * (2 * depth + lanes),
            bytes_accessed=2 * chans * (owners * per_owner * depth + depth * times + owners * lanes),
            transcendentals=0,
        ),
        name="beam_power",
    )(*volts, rows, onehot, inverse, flag, width)


def body(voltages, beam_weights, flags, sk_bins, bin_of_sample):
    dish_count = lax.axis_size("dish")
    chan_count = lax.axis_size("chan")
    _, inside, chan_block, times = voltages.shape
    chans = chan_block // dish_count
    samples = float(inside * dish_count * times)
    owners = dish_count * chan_count
    per_owner = beam_weights.shape[3] // owners

    me = lax.axis_index("dish")
    here = jnp.reshape(me, (1,))
    order = tuple(sorted(range(dish_count), key=distance, reverse=True))
    arrived = []
    for step, block in zip(order, turned_blocks(voltages, here, order)):
        pairs = [(d, relative(d, step, 1)) for d in range(dish_count)]
        arrived.append(lax.ppermute(block, "dish", pairs) if step else block)

    offset = lax.axis_index("dish") * chans
    flag = lax.dynamic_slice_in_dim(flags, offset, chans).astype(jnp.float32)
    width = 0.05 * lax.dynamic_slice_in_dim(sk_bins, offset, chans).astype(jnp.float32)
    matches = bin_of_sample[:, None] == jnp.arange(TBINS, dtype=jnp.int32)[None, :]
    inverse = jnp.tile(1.0 / jnp.sum(matches.astype(jnp.float32), axis=0), per_owner)[None, :]
    lane = jnp.arange(per_owner * TBINS, dtype=jnp.int32)
    place = jnp.arange(per_owner, dtype=jnp.int32)[:, None, None] * TBINS + bin_of_sample[None, :, None]
    onehot = (place == lane[None, None, :]).astype(jnp.bfloat16).reshape(per_owner * times, -1)

    tables = (onehot, inverse, flag[:, None, None], width[:, None, None])
    beam_weights, *tables = lax.optimization_barrier((beam_weights, *tables))
    rows = weight_rows(beam_weights, here, order, per_owner, dish_count, chan_count)
    rows = rows.reshape(chans, per_owner, owners, -1)

    power = beam_power(samples, arrived, rows, *tables)
    blocks = power.reshape(chans, dish_count, chan_count, -1).transpose(2, 1, 0, 3)
    moved = lax.all_to_all(
        blocks.reshape(owners, chans, -1), ("chan", "dish"), split_axis=0, concat_axis=0, tiled=True
    )
    return moved.reshape(owners * chans, -1)


def solution(mesh):
    in_specs = (
        P(None, "dish", "chan", None),
        P(None, ("chan", "dish"), None, None),
        P("chan"),
        P("chan"),
        P(),
    )
    out_specs = P(None, ("dish", "chan"))
    return jax.shard_map(body, mesh=mesh, in_specs=in_specs, out_specs=out_specs, check_vma=False)
```

```python
import functools

import jax
import jax.numpy as jnp
from jax import lax
from jax.experimental import pallas as pl
from jax.experimental.pallas import tpu as pltpu
from jax.sharding import PartitionSpec as P

TBINS = 64
STEP = 4
ROW = 4
DISHES = 8
LANES = 128
VMEM_LIMIT = 46 * 1024 * 1024


def relative(index, step, sign):
    rows = DISHES // ROW
    across = (index % ROW + sign * (step % ROW) + ROW) % ROW
    return (index // ROW + step // ROW) % rows * ROW + across


def distance(step):
    across = step % ROW
    return 4 * (step // ROW) + min(across, ROW - across)


def turn_kernel(order, me_ref, volts_ref, *refs):
    *outs, came_ref, floats_ref, turned_ref, in_sems, out_sems = refs
    count, parts, inside, chans, times = came_ref.shape
    loads, stores = [], []
    for k in range(count):
        start = pl.multiple_of(relative(me_ref[0], order[k], 1) * chans, chans)
        block = volts_ref.at[:, :, pl.ds(start, chans), :]
        loads.append(pltpu.make_async_copy(block, came_ref.at[k], in_sems.at[k]))
        stores.append(pltpu.make_async_copy(turned_ref.at[k], outs[k], out_sems.at[k]))
    for load in loads:
        load.start()
    for k in range(count):
        loads[k].wait()
        block = came_ref[k].astype(jnp.float32).reshape(parts * inside * chans, times)
        for tile in range(times // LANES):
            floats_ref[k % 2, tile] = block[:, tile * LANES : (tile + 1) * LANES]
        for tile in range(times // LANES):
            lanes = slice(tile * LANES, (tile + 1) * LANES)
            for chan in range(chans):
                rows = floats_ref[k % 2, tile, pl.ds(chan, parts * inside, stride=chans), :]
                turned_ref[k, chan, :, lanes] = rows.astype(jnp.bfloat16)
        stores[k].start()
    for store in stores:
        store.wait()


def turned_blocks(volts, me, order):
    parts, inside, chan_block, times = volts.shape
    count = len(order)
    chans = chan_block // count
    shape = (chans, parts * inside, times)
    return pl.pallas_call(
        functools.partial(turn_kernel, order),
        in_specs=[pl.BlockSpec(memory_space=pltpu.SMEM), pl.BlockSpec(memory_space=pl.ANY)],
        out_specs=[pl.BlockSpec(memory_space=pl.ANY)] * count,
        out_shape=[jax.ShapeDtypeStruct(shape, jnp.bfloat16)] * count,
        scratch_shapes=[
            pltpu.VMEM((count, parts, inside, chans, times), jnp.bfloat16),
            pltpu.VMEM((2, times // LANES, parts * inside * chans, LANES), jnp.float32),
            pltpu.VMEM((count, *shape), jnp.bfloat16),
            pltpu.SemaphoreType.DMA((count,)),
            pltpu.SemaphoreType.DMA((count,)),
        ],
        compiler_params=pltpu.CompilerParams(vmem_limit_bytes=63 * 1024 * 1024),
        name="turned_blocks",
    )(me, volts)


def weight_rows_kernel(order, me_ref, weights_ref, rows_ref):
    owners = len(order)
    per_owner = rows_ref.shape[1]
    span = rows_ref.shape[3]
    block = per_owner * span
    inside = weights_ref.shape[2] // owners
    stacked = []
    for part in range(2):
        for step in order:
            start = pl.multiple_of(relative(me_ref[0], step, -1) * inside, inside)
            stacked.append(weights_ref[part, 0, pl.ds(start, inside), :])
    stacked = jnp.concatenate(stacked, axis=0)
    new = lax.broadcasted_iota(jnp.int32, (block, block), 0)
    old = lax.broadcasted_iota(jnp.int32, (block, block), 1)
    wanted = (new % span) * per_owner + new // span
    pick = (wanted == old).astype(jnp.bfloat16)
    for at in range(owners):
        piece = stacked[:, at * block : (at + 1) * block]
        turned = lax.dot_general(
            pick, piece, (((1,), (1,)), ((), ())), preferred_element_type=jnp.float32
        ).astype(jnp.bfloat16)
        for j in range(per_owner):
            rows_ref[0, j, at] = turned[j * span : (j + 1) * span]


def weight_rows(weights, me, order, per_owner, dish_count, chan_count):
    _, chans, dishes, beams = weights.shape
    shape = (chans, per_owner, dish_count, chan_count, 2 * dishes)
    return pl.pallas_call(
        functools.partial(weight_rows_kernel, order),
        grid=(chans,),
        in_specs=[
            pl.BlockSpec(memory_space=pltpu.SMEM),
            pl.BlockSpec((2, 1, dishes, beams), lambda c: (0, c, 0, 0)),
        ],
        out_specs=pl.BlockSpec((1, *shape[1:]), lambda c: (c, 0, 0, 0, 0)),
        out_shape=jax.ShapeDtypeStruct(shape, jnp.bfloat16),
        compiler_params=pltpu.CompilerParams(vmem_limit_bytes=VMEM_LIMIT),
        cost_estimate=pl.CostEstimate(
            flops=2 * chans * beams * 128 * 2 * dishes,
            bytes_accessed=8 * chans * beams * dishes,
            transcendentals=0,
        ),
        name="weight_rows",
    )(me, weights)


def channel_power(samples, at, refs):
    *volts_refs, rows_ref, onehot_ref, inverse_ref, flag_ref, width_ref = refs
    _, both, times = volts_refs[0].shape
    half = both // 2
    real = jnp.concatenate([ref[at, :half] for ref in volts_refs], axis=0)
    imag = jnp.concatenate([ref[at, half:] for ref in volts_refs], axis=0)
    real_f, imag_f = real.astype(jnp.float32), imag.astype(jnp.float32)
    power = real_f * real_f + imag_f * imag_f
    first = jnp.sum(jnp.sum(power, axis=1, keepdims=True), axis=0, keepdims=True)
    second = jnp.sum(jnp.sum(power * power, axis=1, keepdims=True), axis=0, keepdims=True)
    mean_one = first / samples
    mean_two = second / samples
    ratio = mean_two / (mean_one * mean_one + 1e-06)
    kurtosis = (samples + 1.0) / (samples - 1.0) * (ratio - 1.0)
    excess = kurtosis - 1.0
    widths = width_ref[at]
    scaling = flag_ref[at] * widths / (widths + excess * excess)
    gain = (scaling * scaling) * inverse_ref[...]
    stacked = jnp.concatenate(
        [jnp.concatenate([real, imag], axis=1), jnp.concatenate([-imag, real], axis=1)], axis=0
    )
    detected = []
    for j in range(rows_ref.shape[1]):
        beams = jnp.dot(rows_ref[at, j], stacked, preferred_element_type=jnp.float32)
        re, im = beams[:, :times], beams[:, times:]
        detected.append((re * re + im * im).astype(jnp.bfloat16))
    summed = jnp.dot(
        jnp.concatenate(detected, axis=1), onehot_ref[...], preferred_element_type=jnp.float32
    )
    return summed * gain


def beam_kernel(samples, *refs):
    *operands, out_ref = refs
    for at in range(STEP):
        out_ref[at] = channel_power(samples, at, operands).astype(jnp.bfloat16)


def beam_power(samples, volts, rows, onehot, inverse, flag, width):
    chans, both, times = volts[0].shape
    _, per_owner, owners, depth = rows.shape
    lanes = onehot.shape[1]
    whole = lambda *dims: pl.BlockSpec(dims, lambda c: (0,) * len(dims))
    return pl.pallas_call(
        functools.partial(beam_kernel, samples),
        grid=(chans // STEP,),
        in_specs=[
            *[pl.BlockSpec((STEP, both, times), lambda c: (c, 0, 0))] * len(volts),
            pl.BlockSpec((STEP, per_owner, owners, depth), lambda c: (c, 0, 0, 0)),
            whole(*onehot.shape),
            whole(*inverse.shape),
            pl.BlockSpec((STEP, 1, 1), lambda c: (c, 0, 0)),
            pl.BlockSpec((STEP, 1, 1), lambda c: (c, 0, 0)),
        ],
        out_specs=pl.BlockSpec((STEP, owners, lanes), lambda c: (c, 0, 0)),
        out_shape=jax.ShapeDtypeStruct((chans, owners, lanes), jnp.bfloat16),
        compiler_params=pltpu.CompilerParams(vmem_limit_bytes=VMEM_LIMIT),
        cost_estimate=pl.CostEstimate(
            flops=2 * chans * owners * per_owner * times * (2 * depth + lanes),
            bytes_accessed=2 * chans * (owners * per_owner * depth + depth * times + owners * lanes),
            transcendentals=0,
        ),
        name="beam_power",
    )(*volts, rows, onehot, inverse, flag, width)


def body(voltages, beam_weights, flags, sk_bins, bin_of_sample):
    dish_count = lax.axis_size("dish")
    chan_count = lax.axis_size("chan")
    _, inside, chan_block, times = voltages.shape
    chans = chan_block // dish_count
    samples = float(inside * dish_count * times)
    owners = dish_count * chan_count
    per_owner = beam_weights.shape[3] // owners

    me = lax.axis_index("dish")
    here = jnp.reshape(me, (1,))
    order = tuple(sorted(range(dish_count), key=distance, reverse=True))
    arrived = []
    for step, block in zip(order, turned_blocks(voltages, here, order)):
        pairs = [(d, relative(d, step, 1)) for d in range(dish_count)]
        arrived.append(lax.ppermute(block, "dish", pairs) if step else block)

    offset = lax.axis_index("dish") * chans
    flag = lax.dynamic_slice_in_dim(flags, offset, chans).astype(jnp.float32)
    width = 0.05 * lax.dynamic_slice_in_dim(sk_bins, offset, chans).astype(jnp.float32)
    matches = bin_of_sample[:, None] == jnp.arange(TBINS, dtype=jnp.int32)[None, :]
    inverse = jnp.tile(1.0 / jnp.sum(matches.astype(jnp.float32), axis=0), per_owner)[None, :]
    lane = jnp.arange(per_owner * TBINS, dtype=jnp.int32)
    place = jnp.arange(per_owner, dtype=jnp.int32)[:, None, None] * TBINS + bin_of_sample[None, :, None]
    onehot = (place == lane[None, None, :]).astype(jnp.bfloat16).reshape(per_owner * times, -1)

    tables = (onehot, inverse, flag[:, None, None], width[:, None, None])
    beam_weights, *tables = lax.optimization_barrier((beam_weights, *tables))
    rows = weight_rows(beam_weights, here, order, per_owner, dish_count, chan_count)
    rows = rows.reshape(chans, per_owner, owners, -1)

    power = beam_power(samples, arrived, rows, *tables)
    blocks = power.reshape(chans, dish_count, chan_count, -1).transpose(2, 1, 0, 3)
    moved = lax.all_to_all(
        blocks.reshape(owners, chans, -1), ("chan", "dish"), split_axis=0, concat_axis=0, tiled=True
    )
    return moved.reshape(owners * chans, -1)


def solution(mesh):
    in_specs = (
        P(None, "dish", "chan", None),
        P(None, ("chan", "dish"), None, None),
        P("chan"),
        P("chan"),
        P(),
    )
    out_specs = P(None, ("dish", "chan"))
    return jax.shard_map(body, mesh=mesh, in_specs=in_specs, out_specs=out_specs, check_vma=False)
```
